32 devices in a mesh: dp: 4 (over x, y), tp: 8 (over z, core).
Axes of the slice: x: 2, y: 2, z: 4, core: 2. Of those that a mesh axis runs over, the one named last changes fastest.
Arguments:
- x: bfloat16 [8192, 12288], P('dp'), parts along dimension 0
- gain: bfloat16 [12288], replicated
- wq: bfloat16 [12288, 12288], P(None, 'tp')
- wk: bfloat16 [12288, 1024], P(None, 'tp')
- wv: bfloat16 [12288, 1024], P(None, 'tp')
- wo: bfloat16 [12288, 12288], P('tp')
Outputs:
- output: bfloat16 [8192, 12288], P('dp'), parts along dimension 0
There are 4 independent parts. The reference program is written for one: setup_inputs(seed, part) draws one part's arguments, and reference() takes and returns one part's arrays. A program takes and returns all parts, laid end to end along the dimension named above; an argument that names none is the same for every part.
All inputs are finite; a program needn't handle non-finite values.
Results may differ from the reference program's by a relative error of at most 0.012.
Values are sent between devices in bfloat16 or wider.
A program may use at most 2 GiB of HBM per device.

```python
import jax
import jax.numpy as jnp
from jax import lax

ROWS = 2048
D = 12288
HEADS = 96
KV_HEADS = 8
HEAD = 128
THETA = 10000


def setup_inputs(seed: int = 0, part: int = 0) -> dict:
    kx, kn, kq, kk, kv, ko = jax.random.split(jax.random.key(seed), 6)

    def weights(key, rows, columns):
        return jax.random.normal(key, (rows, columns), jnp.float32) * rows**-0.5

    drawn = {
        "x": jax.random.normal(jax.random.fold_in(kx, part), (ROWS, D), jnp.float32),
        "gain": 1 + 0.1 * jax.random.normal(kn, (D,), jnp.float32),
        "wq": 2 * weights(kq, D, HEADS * HEAD),
        "wk": 2 * weights(kk, D, KV_HEADS * HEAD),
        "wv": 4 * weights(kv, D, KV_HEADS * HEAD),
        "wo": weights(ko, HEADS * HEAD, D),
    }
    return {k: v.astype(jnp.bfloat16) for k, v in drawn.items()}


def normed(x, gain):
    wide = x.astype(jnp.float32)
    scale = lax.rsqrt(jnp.mean(wide * wide, -1, keepdims=True) + 1e-6)
    return (wide * scale * gain.astype(jnp.float32)).astype(jnp.bfloat16)


def turned(t, place, theta):
    half = t.shape[-1] // 2
    angle = place.astype(jnp.float32)[:, None] * theta ** (-jnp.arange(half, dtype=jnp.float32) / half)
    cos, sin = jnp.cos(angle)[:, None], jnp.sin(angle)[:, None]
    a, b = t[..., :half].astype(jnp.float32), t[..., half:].astype(jnp.float32)
    return jnp.concatenate([a * cos - b * sin, b * cos + a * sin], -1).astype(jnp.bfloat16)


def matmul(a, w):
    return jnp.dot(a, w, preferred_element_type=jnp.float32).astype(jnp.bfloat16)


def einsum(form, a, b):
    return jnp.einsum(form, a.astype(jnp.float32), b.astype(jnp.float32))


def attention(q, k, v):
    scores = einsum("tgsd,ugd->gstu", q, k) * q.shape[-1] ** -0.5
    token = jnp.arange(q.shape[0])
    scores = jnp.where(token[:, None] >= token, scores, -jnp.inf)
    weights = jax.nn.softmax(scores, -1).astype(jnp.bfloat16)
    return einsum("gstu,ugd->tgsd", weights, v).astype(jnp.bfloat16)


def reference(x, gain, wq, wk, wv, wo):
    a, place = normed(x, gain), jnp.arange(ROWS)
    q = turned(matmul(a, wq).reshape(ROWS, HEADS, HEAD), place, THETA).reshape(ROWS, KV_HEADS, -1, HEAD)
    k = turned(matmul(a, wk).reshape(ROWS, KV_HEADS, HEAD), place, THETA)
    v = matmul(a, wv).reshape(ROWS, KV_HEADS, HEAD)
    seen = attention(q, k, v).reshape(ROWS, HEADS * HEAD)
    return (x.astype(jnp.float32) + jnp.dot(seen, wo, preferred_element_type=jnp.float32)).astype(jnp.bfloat16)
```

```python
import functools

import numpy as np

import jax
import jax.numpy as jnp
from jax import lax
from jax.experimental import pallas as pl
from jax.experimental.pallas import tpu as pltpu
from jax.sharding import PartitionSpec as P

HEAD = 128
THETA = 10000
NEG = -1e30
HIDDEN = 2 * NEG
LOG2E = 1.4426950408889634
MESH = pl.DeviceIdType.MESH
F32, BF16 = jnp.float32, jnp.bfloat16

STEPS = 12
PROJ = 6
L1, L2, L3, L4, L5 = 1, 3, 5, 7, 9


def _dot(a, b, ca=1, cb=0):
    return lax.dot_general(a, b, (((ca,), (cb,)), ((), ())), preferred_element_type=F32)


def _kernel(x, gain, trig, wq, wk, wv, wo, y, xc, a_s, acc, scl, wqb, wkvb, wob, q_s, k_s, vt_s, seen, mix, top_s,
            tsend, trecv, own, psend, precv, ssend, mrecv, xres, ybuf,
            sx, sw, swo, sxr, s_t, r_t, s_p, r_p, s_m, r_m, s_yl, s_yp, s_yo, r_y, s_f, r_f):
    rows, wide = x.shape
    chunk = xc.shape[0]
    heads = q_s.shape[0]
    chunks = rows // chunk
    kb, nb = wide // PROJ, wide // STEPS
    half = nb // 2
    hs = heads // (STEPS - PROJ)
    units = chunks * STEPS
    e = HEAD**-0.5 * LOG2E

    me = lax.axis_index("tp")
    z, c = lax.div(me, 2), lax.rem(me, 2)
    inner = (z == 1) | (z == 2)
    outer = jnp.logical_not(inner)
    partner = {"tp": 2 * z + 1 - c}
    near = {"tp": 2 * (z + 1 - 2 * lax.rem(z, 2)) + c}
    far = {"tp": 2 * jnp.clip(3 - z, 1, 2) + c}

    def rem(v, n):
        return lax.rem(v, n)

    def remote(src, dst, ssem, rsem, to):
        return pltpu.make_async_remote_copy(src_ref=src, dst_ref=dst, send_sem=ssem, recv_sem=rsem, device_id=to, device_id_type=MESH)

    def place(v):
        r = pl.multiple_of(lax.div(v, STEPS) * chunk, chunk)
        k = pl.multiple_of(rem(v, STEPS) * nb + c * half, half)
        return pl.ds(r, chunk), pl.ds(k, half)

    def mine(v):
        r, k = place(v)
        return y.at[r, k]

    def x_copy(p):
        return pltpu.make_async_copy(x.at[pl.ds(pl.multiple_of(p * chunk, chunk), chunk), :], xc, sx)

    def w_copies(s):
        k, b = pl.ds(pl.multiple_of(rem(s, PROJ) * kb, kb), kb), rem(s, 2)
        return [pltpu.make_async_copy(wq.at[k, :], wqb.at[b], sw.at[0, b]),
                pltpu.make_async_copy(wk.at[k, :], wkvb.at[b, :, pl.ds(0, HEAD)], sw.at[1, b]),
                pltpu.make_async_copy(wv.at[k, :], wkvb.at[b, :, pl.ds(HEAD, HEAD)], sw.at[2, b])]

    def wo_copy(v):
        return pltpu.make_async_copy(wo.at[:, pl.ds(pl.multiple_of(rem(v, STEPS) * nb, nb), nb)], wob.at[rem(v, 2)], swo.at[rem(v, 2)])

    def xres_copy(v):
        r, k = place(v)
        return pltpu.make_async_copy(x.at[r, k], xres.at[rem(v, 3)], sxr.at[rem(v, 3)])

    def t_copy(v):
        return remote(tsend.at[rem(v, 2)], trecv.at[rem(v, 4)], s_t.at[rem(v, 2)], r_t.at[rem(v, 4)], partner)

    def p_copy(v):
        return remote(psend.at[rem(v, 4)], precv.at[rem(v, 7)], s_p.at[rem(v, 4)], r_p.at[rem(v, 7)], near)

    def m_copy(v):
        return remote(ssend.at[rem(v, 4)], mrecv.at[rem(v, 6)], s_m.at[rem(v, 4)], r_m.at[rem(v, 6)], far)

    def yl_copy(v):
        return pltpu.make_async_copy(ybuf.at[rem(v, 4)], mine(v), s_yl.at[rem(v, 4)])

    def yp_copy(v):
        return remote(ybuf.at[rem(v, 4)], mine(v), s_yp.at[rem(v, 4)], r_f.at[rem(v, 16)], partner)

    def yo_copy(v):
        return remote(ybuf.at[rem(v, 4)], mine(v), s_yo.at[rem(v, 4)], r_y.at[rem(v, 8)], near)

    def f_copy(v):
        return remote(mine(v), mine(v), s_f.at[rem(v, 8)], r_f.at[rem(v, 16)], partner)

    def squares(first, count, start):
        def some(n, t):
            v = xc[:, pl.ds(pl.multiple_of(first + n * 128, 128), 128)].astype(F32)
            return t + v * v
        scl[...] = lax.fori_loop(0, count // 128, some, start)

    def scales():
        t = jnp.sum(scl[...], axis=1, keepdims=True)
        scl[...] = jnp.broadcast_to(lax.rsqrt(t * (1 / wide) + 1e-6), scl.shape)

    def rotated(t, cos, sin):
        t = t.astype(BF16).astype(F32)
        return (t * cos + pltpu.roll(t, HEAD // 2, 1) * sin).astype(BF16)

    def project(p, i):
        s = p * PROJ + i
        b = rem(s, 2)
        for w in w_copies(s):
            w.wait()
        k = pl.ds(pl.multiple_of(i * kb, kb), kb)
        a_s[...] = (xc[:, k].astype(F32) * scl[:, :1] * gain[:, k].astype(F32)).astype(BF16)
        n_w = min(512, heads * HEAD)

        def some(n, _):
            at = pl.ds(pl.multiple_of(n * n_w, n_w), n_w)
            d = _dot(a_s[...], wqb[b, :, at])
            acc[:, at] = jnp.where(i == 0, d, acc[:, at] + d)

        lax.fori_loop(0, heads * HEAD // n_w, some, None)
        at = pl.ds(heads * HEAD, 2 * HEAD)
        d = _dot(a_s[...], wkvb[b])
        acc[:, at] = jnp.where(i == 0, d, acc[:, at] + d)

        @pl.when(i == PROJ - 1)
        def _():
            @pl.when(p + 1 < chunks)
            def _():
                x_copy(p + 1).start()

            here = pl.ds(pl.multiple_of(p * chunk, chunk), chunk)
            cs = trig[here, :]
            swapped = pltpu.roll(cs, HEAD // 2, 1)
            low = lax.broadcasted_iota(jnp.int32, cs.shape, 1) < HEAD // 2
            cos, sin = jnp.where(low, cs, swapped), jnp.where(low, -swapped, cs)

            def head(h, _):
                q_s[h] = rotated(acc[:, pl.ds(pl.multiple_of(h * HEAD, HEAD), HEAD)], cos, sin)

            lax.fori_loop(0, heads, head, None)
            k_s[here, :] = rotated(acc[:, pl.ds(heads * HEAD, HEAD)], cos, sin)
            vt_s[:HEAD, here] = acc[:, pl.ds(heads * HEAD + HEAD, HEAD)].T.astype(BF16)

    def attend(p, i):
        first = (i - PROJ) * hs
        q = q_s[pl.ds(first, hs)].reshape(hs * chunk, HEAD)
        top_s[...] = jnp.full(top_s.shape, NEG, F32)
        mix[...] = jnp.zeros(mix.shape, F32)

        def block(j, masked):
            here = pl.ds(pl.multiple_of(j * chunk, chunk), chunk)
            s = _dot(k_s[here, :], q, 1, 1)
            if masked:
                query = lax.rem(lax.broadcasted_iota(jnp.int32, s.shape, 1), chunk)
                s = jnp.where(lax.broadcasted_iota(jnp.int32, s.shape, 0) <= query, s, HIDDEN)
            old = top_s[:1, :]
            top = jnp.maximum(old, s.max(axis=0, keepdims=True))
            top_s[:1, :] = top
            w = jnp.exp2((s - top) * e).astype(BF16)
            mix[...] = mix[...] * jnp.exp2((old - top) * e) + _dot(vt_s[:, here], w)

        lax.fori_loop(0, p, lambda j, _: block(j, False), None)
        block(p, True)
        out = (mix[:HEAD, :] * (1 / mix[HEAD : HEAD + 1, :])).T.astype(BF16)
        for n in range(hs):
            seen[rem(p, 2), :, pl.ds(pl.multiple_of((first + n) * HEAD, HEAD), HEAD)] = out[n * chunk : (n + 1) * chunk]

    x_copy(0).start()
    for w in w_copies(0):
        w.start()
    barrier = pltpu.get_barrier_semaphore()
    pl.semaphore_signal(barrier, inc=1, device_id=partner, device_id_type=MESH)
    pl.semaphore_signal(barrier, inc=1, device_id=near, device_id_type=MESH)

    @pl.when(inner)
    def _():
        pl.semaphore_signal(barrier, inc=1, device_id=far, device_id_type=MESH)
        pl.semaphore_wait(barrier, 3)

    @pl.when(outer)
    def _():
        pl.semaphore_wait(barrier, 2)

    vt_s[HEAD:, :] = jnp.ones((vt_s.shape[0] - HEAD, rows), BF16)
    x_copy(0).wait()
    squares(0, wide, jnp.zeros(scl.shape, F32))
    scales()

    def step(g, _):
        p, i = lax.div(g, STEPS), rem(g, STEPS)
        u = g - STEPS

        def at(lag, also=None):
            def run(f):
                v = u - lag
                ok = (v >= 0) & (v < units)
                pl.when(ok if also is None else ok & also)(lambda: f(v))
            return run

        @pl.when((i < PROJ) & (p * PROJ + i + 1 < chunks * PROJ))
        def _():
            for w in w_copies(p * PROJ + i + 1):
                w.start()

        @at(-1)
        def _(v):
            wo_copy(v).start()

        @at(L3 - 2, inner)
        def _(v):
            xres_copy(v).start()

        @at(2)
        def _(v):
            t_copy(v).wait_send()

        @at(0)
        def _(v):
            wo_copy(v).wait()
            part = pl.ds(pl.multiple_of((1 - c) * half, half), half)
            tsend[rem(v, 2)] = _dot(seen[rem(lax.div(v, STEPS), 2)], wob[rem(v, 2), :, part]).astype(BF16)
            t_copy(v).start()

        @at(L1 + 4, outer)
        def _(v):
            p_copy(v).wait_send()

        @at(L1)
        def _(v):
            t_copy(v).wait_recv()
            total = own[rem(v, 4)] + trecv[rem(v, 4)].astype(F32)

            @pl.when(outer)
            def _():
                psend[rem(v, 4)] = total.astype(BF16)
                p_copy(v).start()

            @pl.when(inner)
            def _():
                own[rem(v, 4)] = total

        @at(L2 + 4, inner)
        def _(v):
            m_copy(v).wait_send()

        @at(L2, inner)
        def _(v):
            p_copy(v).wait_recv()
            ssend[rem(v, 4)] = (own[rem(v, 4)] + precv[rem(v, 7)].astype(F32)).astype(BF16)
            m_copy(v).start()

        @at(L3 + 4, inner)
        def _(v):
            yl_copy(v).wait()
            yp_copy(v).wait_send()
            yo_copy(v).wait_send()

        @at(L3, inner)
        def _(v):
            m_copy(v).wait_recv()
            xres_copy(v).wait()
            total = ssend[rem(v, 4)].astype(F32) + mrecv[rem(v, 6)].astype(F32)
            ybuf[rem(v, 4)] = (xres[rem(v, 3)].astype(F32) + total).astype(BF16)
            yo_copy(v).start()
            yp_copy(v).start()
            yl_copy(v).start()

        @at(L4, outer)
        def _(v):
            yo_copy(v).wait_recv()
            f_copy(v).start()

        @at(0)
        def _(v):
            part = pl.ds(pl.multiple_of(c * half, half), half)
            own[rem(v, 4)] = _dot(seen[rem(lax.div(v, STEPS), 2)], wob[rem(v, 2), :, part])

        @pl.when((p < chunks) & (i < PROJ))
        def _():
            project(p, i)

        @pl.when((p < chunks) & (i >= PROJ))
        def _():
            attend(p, i)

        third = wide // 3
        @pl.when((p + 1 < chunks) & (i >= STEPS - 3))
        def _():
            @pl.when(i == STEPS - 3)
            def _():
                x_copy(p + 1).wait()

            squares((i - STEPS + 3) * third, third, jnp.where(i == STEPS - 3, 0.0, scl[...]))

            @pl.when(i == STEPS - 1)
            def _():
                scales()

        @at(L5, outer)
        def _(v):
            f_copy(v).wait_send()

        @at(L5)
        def _(v):
            f_copy(v).wait_recv()

    lax.fori_loop(0, STEPS + units + L5, step, None)


def _trig(rows):
    half = HEAD // 2
    angle = np.arange(rows, dtype=np.float32)[:, None] * (float(THETA) ** (-np.arange(half) / half)).astype(np.float32)
    angle = angle.astype(np.float64)
    return np.concatenate([np.cos(angle), np.sin(angle)], 1).astype(np.float32)


def layer(x, gain, wq, wk, wv, wo, chunk=256):
    rows, wide = x.shape
    mine = wq.shape[1]
    heads = mine // HEAD
    kb, nb = wide // PROJ, wide // STEPS
    half = nb // 2
    hs = heads // (STEPS - PROJ)
    hbm, vmem = pl.BlockSpec(memory_space=pl.ANY), pl.BlockSpec(memory_space=pltpu.VMEM)

    def slots(n, t=BF16):
        return pltpu.VMEM((n, chunk, half), t)

    dma = pltpu.SemaphoreType.DMA
    return pl.pallas_call(
        _kernel,
        out_shape=jax.ShapeDtypeStruct((rows, wide), BF16),
        in_specs=[hbm, vmem, vmem, hbm, hbm, hbm, hbm],
        out_specs=hbm,
        scratch_shapes=[
            pltpu.VMEM((chunk, wide), BF16), pltpu.VMEM((chunk, kb), BF16), pltpu.VMEM((chunk, mine + 2 * HEAD), F32), pltpu.VMEM((chunk, 128), F32),
            pltpu.VMEM((2, kb, mine), BF16), pltpu.VMEM((2, kb, 2 * HEAD), BF16), pltpu.VMEM((2, mine, nb), BF16),
            pltpu.VMEM((heads, chunk, HEAD), BF16), pltpu.VMEM((rows, HEAD), BF16), pltpu.VMEM((HEAD + 16, rows), BF16),
            pltpu.VMEM((2, chunk, mine), BF16), pltpu.VMEM((HEAD + 16, hs * chunk), F32), pltpu.VMEM((8, hs * chunk), F32),
            slots(2), slots(4), slots(4, F32), slots(4), slots(7), slots(4), slots(6), slots(3), slots(4),
            dma, dma((3, 2)), dma((2,)), dma((3,)), dma((2,)), dma((4,)), dma((4,)), dma((7,)), dma((4,)), dma((6,)),
            dma((4,)), dma((4,)), dma((4,)), dma((8,)), dma((8,)), dma((16,)),
        ],
        compiler_params=pltpu.CompilerParams(collective_id=0, has_side_effects=True, vmem_limit_bytes=60 * 2**20),
        cost_estimate=pl.CostEstimate(flops=4 * rows * wide * (mine + HEAD), transcendentals=heads * rows * rows // 2,
                                      bytes_accessed=8 * 4 * wide * mine),
        name="layer",
    )(x, gain.reshape(1, wide), jnp.asarray(_trig(rows)), wq, wk, wv, wo)


def solution(mesh):
    tokens, columns = P("dp", None), P(None, "tp")
    return jax.shard_map(
        layer,
        mesh=mesh,
        in_specs=(tokens, P(None), columns, columns, columns, P("tp", None)),
        out_specs=tokens,
        check_vma=False,
    )
```

```python
import functools

import numpy as np

import jax
import jax.numpy as jnp
from jax import lax
from jax.experimental import pallas as pl
from jax.experimental.pallas import tpu as pltpu
from jax.sharding import PartitionSpec as P

HEAD = 128
THETA = 10000
NEG = -1e30
HIDDEN = 2 * NEG
LOG2E = 1.4426950408889634
MESH = pl.DeviceIdType.MESH
VMEM = 67043328
F32, BF16 = jnp.float32, jnp.bfloat16

STEPS = 12
TICKS = 4
PROJ = 6
GROUP = 4
QUIET = 2
L1, L2, L3, L4, L5 = 2, 5, 9, 15, 19


def _dot(a, b, ca=1, cb=0):
    return lax.dot_general(a, b, (((ca,), (cb,)), ((), ())), preferred_element_type=F32)


def _kernel(x, gain, trig, wq, wk, wv, wo, y, xc, a_s, acc, scl, g_s, wqb, wkvb, wob, q_s, k_s, vt_s, seen, mix, top_s,
            tsend, trecv, own, psend, precv, ssend, mrecv, xres, ybuf,
            sx, sw, swo, sxr, s_t, r_t, s_p, r_p, s_m, r_m, s_yl, s_yp, s_yo, r_y, s_f, r_f):
    rows, wide = x.shape
    chunk = xc.shape[0]
    heads = q_s.shape[0]
    chunks = rows // chunk
    kb, nb = wide // PROJ, wide // STEPS
    half = nb // 2
    groups = heads // GROUP
    piece = chunk // TICKS
    units = chunks * STEPS
    e = HEAD**-0.5 * LOG2E

    me = lax.axis_index("tp")
    z, c = lax.div(me, 2), lax.rem(me, 2)
    inner = (z == 1) | (z == 2)
    outer = jnp.logical_not(inner)
    partner = {"tp": 2 * z + 1 - c}
    near = {"tp": 2 * (z + 1 - 2 * lax.rem(z, 2)) + c}
    far = {"tp": 2 * jnp.clip(3 - z, 1, 2) + c}
    rem = lax.rem

    def remote(src, dst, ssem, rsem, to):
        return pltpu.make_async_remote_copy(src_ref=src, dst_ref=dst, send_sem=ssem, recv_sem=rsem, device_id=to, device_id_type=MESH)

    def place(v, n=None):
        r = pl.multiple_of(lax.div(v, STEPS) * chunk, chunk)
        k = pl.multiple_of(rem(v, STEPS) * nb + c * half, half)
        return (pl.ds(r, chunk) if n is None else pl.ds(r + n * piece, piece)), pl.ds(k, half)

    def mine(v, n):
        r, k = place(v, n)
        return y.at[r, k]

    def part_of(n):
        return pl.ds(n * piece, piece)

    def x_copies(p):
        w = wide // 4
        return [pltpu.make_async_copy(x.at[pl.ds(pl.multiple_of(p * chunk, chunk), chunk), pl.ds(n * w, w)], xc.at[:, pl.ds(n * w, w)], sx.at[n])
                for n in range(4)]

    def w_copies(s):
        k, b = pl.ds(pl.multiple_of(rem(s, PROJ) * kb, kb), kb), rem(s, 3)
        return [pltpu.make_async_copy(wq.at[k, :], wqb.at[b], sw.at[0, b]),
                pltpu.make_async_copy(wk.at[k, :], wkvb.at[b, :, pl.ds(0, HEAD)], sw.at[1, b]),
                pltpu.make_async_copy(wv.at[k, :], wkvb.at[b, :, pl.ds(HEAD, HEAD)], sw.at[2, b])]

    def wo_copy(v):
        return pltpu.make_async_copy(wo.at[:, pl.ds(pl.multiple_of(rem(v, STEPS) * nb, nb), nb)], wob.at[rem(v, 3)], swo.at[rem(v, 3)])

    def xres_copy(v):
        r, k = place(v)
        return pltpu.make_async_copy(x.at[r, k], xres.at[rem(v, 3)], sxr.at[rem(v, 3)])

    def t_copy(v):
        return remote(tsend.at[rem(v, 2)], trecv.at[rem(v, 4)], s_t.at[rem(v, 2)], r_t.at[rem(v, 4)], partner)

    def p_copy(v, n):
        k, j = rem(v, 2), rem(v, 4)
        return remote(psend.at[k, part_of(n)], precv.at[j, part_of(n)], s_p.at[k, n], r_p.at[j, n], near)

    def m_copy(v, n):
        k, j = rem(v, 2), rem(v, 4)
        return remote(ssend.at[k, part_of(n)], mrecv.at[j, part_of(n)], s_m.at[k, n], r_m.at[j, n], far)

    def yl_copy(v, n):
        return pltpu.make_async_copy(ybuf.at[rem(v, 2), part_of(n)], mine(v, n), s_yl.at[rem(v, 2), n])

    def yp_copy(v, n):
        return remote(ybuf.at[rem(v, 2), part_of(n)], mine(v, n), s_yp.at[rem(v, 2), n], r_f.at[rem(v, 8), n], partner)

    def yo_copy(v, n):
        return remote(ybuf.at[rem(v, 2), part_of(n)], mine(v, n), s_yo.at[rem(v, 2), n], r_y.at[rem(v, 8), n], near)

    def f_copy(v, n):
        return remote(mine(v, n), mine(v, n), s_f.at[rem(v, 2), n], r_f.at[rem(v, 8), n], partner)

    def squares(first, count, start):
        def some(n, t):
            v = [xc[:, pl.ds(pl.multiple_of(n * 512, 512) + k * 128, 128)].astype(F32) for k in range(4)]
            return t + ((v[0] * v[0] + v[1] * v[1]) + (v[2] * v[2] + v[3] * v[3]))
        scl[...] = lax.fori_loop(first, first + count, some, start)

    def scales():
        t = jnp.sum(scl[...], axis=1, keepdims=True)
        scl[...] = jnp.broadcast_to(lax.rsqrt(t * (1 / wide) + 1e-6), scl.shape)

    def rotated(t, cos, sin):
        t = t.astype(BF16).astype(F32)
        return (t * cos + pltpu.roll(t, HEAD // 2, 1) * sin).astype(BF16)

    def project(p, i, ticks):
        s = p * PROJ + i
        b = rem(s, 3)
        n_w = 512
        if 1 in ticks:
            for n in range(kb // 128):
                k = pl.ds(pl.multiple_of(i * kb + n * 128, 128), 128)
                a_s[:, n * 128 : (n + 1) * 128] = (xc[:, k].astype(F32) * scl[...] * g_s[pl.ds(i * (kb // 128) + n, 1), :]).astype(BF16)
            for w in w_copies(s):
                w.wait()
        for n in range(heads * HEAD // n_w):
            if n + 1 in ticks:
                at = pl.ds(n * n_w, n_w)
                d = _dot(a_s[...], wqb[b, :, at])
                acc[:, at] = jnp.where(i == 0, d, acc[:, at] + d)
        if 3 in ticks:
            at = pl.ds(heads * HEAD, 2 * HEAD)
            d = _dot(a_s[...], wkvb[b])
            acc[:, at] = jnp.where(i == 0, d, acc[:, at] + d)

    def projected(p):
        here = pl.ds(pl.multiple_of(p * chunk, chunk), chunk)
        cs = trig[here, :]
        swapped = pltpu.roll(cs, HEAD // 2, 1)
        low = lax.broadcasted_iota(jnp.int32, cs.shape, 1) < HEAD // 2
        cos, sin = jnp.where(low, cs, swapped), jnp.where(low, -swapped, cs)

        def head(h, _):
            q_s[h] = rotated(acc[:, pl.ds(pl.multiple_of(h * HEAD, HEAD), HEAD)], cos, sin)

        k_s[here, :] = rotated(acc[:, pl.ds(heads * HEAD, HEAD)], cos, sin)
        vt_s[:HEAD, here] = acc[:, pl.ds(heads * HEAD + HEAD, HEAD)].T.astype(BF16)
        lax.fori_loop(0, heads, head, None)

    def attend(p, group, ticks):
        strips = [group * GROUP + n for n in range(0, GROUP, 2)]

        def block(j, masked):
            here = pl.ds(pl.multiple_of(j * chunk, chunk), chunk)
            scores = [_dot(k_s[here, :], q_s[pl.ds(h, 2)].reshape(2 * chunk, HEAD), 1, 1) for h in strips]
            if masked:
                query = rem(lax.broadcasted_iota(jnp.int32, scores[0].shape, 1), chunk)
                ok = lax.broadcasted_iota(jnp.int32, scores[0].shape, 0) <= query
                scores = [jnp.where(ok, s, HIDDEN) for s in scores]
            weights, keeps = [], []
            for n, s in enumerate(scores):
                old = top_s[n : n + 1, :]
                top = jnp.maximum(old, s.max(axis=0, keepdims=True))
                top_s[n : n + 1, :] = top
                weights.append(jnp.exp2((s - top) * e).astype(BF16))
                keeps.append(jnp.exp2((old - top) * e))
            for n, (w, keep) in enumerate(zip(weights, keeps)):
                mix[n] = mix[n] * keep + _dot(vt_s[:, here], w)

        if 0 in ticks:
            top_s[...] = jnp.full(top_s.shape, NEG, F32)
            mix[...] = jnp.zeros(mix.shape, F32)
        first, last = min(ticks), max(ticks)
        if not isinstance(p, int) or p > 0:
            lo = lax.div((p + 1) * first, TICKS)
            hi = p if last == TICKS - 1 else lax.div((p + 1) * (last + 1), TICKS)
            lax.fori_loop(lo, hi, lambda j, _: block(j, False), None)
        if last == TICKS - 1:
            block(p, True)
            for n, h in enumerate(strips):
                out = (mix[n, :HEAD, :] * (1 / mix[n, HEAD : HEAD + 1, :])).T.astype(BF16)
                for m in range(2):
                    seen[rem(p, 2), :, pl.ds(pl.multiple_of((h + m) * HEAD, HEAD), HEAD)] = out[m * chunk : (m + 1) * chunk]

    xs = x_copies(0)
    xs[0].start()
    xs[1].start()
    barrier = pltpu.get_barrier_semaphore()
    pl.semaphore_signal(barrier, inc=1, device_id=partner, device_id_type=MESH)
    pl.semaphore_signal(barrier, inc=1, device_id=near, device_id_type=MESH)

    @pl.when(inner)
    def _():
        pl.semaphore_signal(barrier, inc=1, device_id=far, device_id_type=MESH)

    g_s[...] = gain[...].astype(F32)
    vt_s[HEAD:, :] = jnp.ones((vt_s.shape[0] - HEAD, rows), BF16)
    scl[...] = jnp.zeros(scl.shape, F32)
    for n in range(4):
        xs[n].wait()
        for more in xs[n + 2 : n + 3] if n < 2 else w_copies(n - 2):
            more.start()
        squares(n * (wide // 2048), wide // 2048, scl[...])
    scales()

    def first_block(i, _):
        @pl.when(i + 2 < chunks * PROJ)
        def _():
            for w in w_copies(i + 2):
                w.start()

        project(0, i, (1, 2, 3))

    lax.fori_loop(0, PROJ, first_block, None)
    for w in x_copies(1) if chunks > 1 else []:
        w.start()
    wo_copy(0).start()
    wo_copy(1).start()
    projected(0)
    lax.fori_loop(0, groups, lambda n, _: attend(0, n, range(TICKS)), None)
    @pl.when(inner)
    def _():
        pl.semaphore_wait(barrier, 3)

    @pl.when(outer)
    def _():
        pl.semaphore_wait(barrier, 2)

    def step(u, _):
        p, i = lax.div(u, STEPS) + 1, rem(u, STEPS)

        k = jnp.where(p == 1, i - QUIET, i)
        projects = (p < chunks) & (k >= 0) & (k < PROJ)
        left = STEPS - i
        group = jnp.where(p == 1, groups - left, groups - lax.div(left + 1, 2))
        attends = (p < chunks) & (group >= 0) & ((p == 1) | (rem(left, 2) == 1))
        adds = (p + 1 < chunks) & (left <= 3)

        for tick in range(TICKS):

            def at(lag, also=None):
                def run(f):
                    v, n = u + (tick - lag) // TICKS, (tick - lag) % TICKS
                    ok = (v >= 0) & (v < units)
                    pl.when(ok if also is None else ok & also)(lambda: f(v, n))
                return run

            if tick == 0:

                @at(-2 * TICKS)
                def _(v, n):
                    wo_copy(v).start()

                @pl.when(projects & (p * PROJ + k + 2 < chunks * PROJ))
                def _():
                    for w in w_copies(p * PROJ + k + 2):
                        w.start()

                @at(TICKS, inner)
                def _(v, n):
                    xres_copy(v).start()

                @at(2 * TICKS)
                def _(v, n):
                    t_copy(v).wait_send()

                @at(0)
                def _(v, n):
                    wo_copy(v).wait()
                    part = pl.ds(pl.multiple_of((1 - c) * half, half), half)
                    tsend[rem(v, 2)] = _dot(seen[rem(lax.div(v, STEPS), 2)], wob[rem(v, 3), :, part]).astype(BF16)
                    t_copy(v).start()

            @at(L1 + 2 * TICKS, outer)
            def _(v, n):
                p_copy(v, n).wait_send()

            @at(L1)
            def _(v, n):
                if n == 0:
                    t_copy(v).wait_recv()
                total = own[rem(v, 4), part_of(n)] + trecv[rem(v, 4), part_of(n)].astype(F32)

                @pl.when(outer)
                def _():
                    psend[rem(v, 2), part_of(n)] = total.astype(BF16)
                    p_copy(v, n).start()

                @pl.when(inner)
                def _():
                    own[rem(v, 4), part_of(n)] = total

            @at(L2 + 2 * TICKS, inner)
            def _(v, n):
                m_copy(v, n).wait_send()

            @at(L2, inner)
            def _(v, n):
                p_copy(v, n).wait_recv()
                ssend[rem(v, 2), part_of(n)] = (own[rem(v, 4), part_of(n)] + precv[rem(v, 4), part_of(n)].astype(F32)).astype(BF16)
                m_copy(v, n).start()

            @at(L3 + 2 * TICKS, inner)
            def _(v, n):
                yl_copy(v, n).wait()
                yp_copy(v, n).wait_send()
                yo_copy(v, n).wait_send()

            @at(L3, inner)
            def _(v, n):
                if n == 0:
                    xres_copy(v).wait()
                m_copy(v, n).wait_recv()
                total = ssend[rem(v, 2), part_of(n)].astype(F32) + mrecv[rem(v, 4), part_of(n)].astype(F32)
                ybuf[rem(v, 2), part_of(n)] = (xres[rem(v, 3), part_of(n)].astype(F32) + total).astype(BF16)
                yo_copy(v, n).start()
                yp_copy(v, n).start()
                yl_copy(v, n).start()

            @at(L4, outer)
            def _(v, n):
                yo_copy(v, n).wait_recv()
                f_copy(v, n).start()

            if tick == 0:

                @at(0)
                def _(v, n):
                    part = pl.ds(pl.multiple_of(c * half, half), half)
                    own[rem(v, 4)] = _dot(seen[rem(lax.div(v, STEPS), 2)], wob[rem(v, 3), :, part])

            else:

                @pl.when(projects)
                def _():
                    project(p, k, (tick,))
                    if tick == TICKS - 1:

                        @pl.when(k == PROJ - 1)
                        def _():
                            @pl.when(p + 1 < chunks)
                            def _():
                                for w in x_copies(p + 1):
                                    w.start()

                            projected(p)

            @pl.when(attends)
            def _():
                attend(p, group, (tick,))

            if tick == TICKS - 1 and chunks > 1:

                @pl.when(u == QUIET - 1)
                def _():
                    for w in x_copies(1):
                        w.wait()
                    squares(0, wide // 512, jnp.zeros(scl.shape, F32))
                    scales()

            if tick == TICKS - 1:
                third = wide // 512 // 3

                @pl.when(adds)
                def _():
                    @pl.when(left == 3)
                    def _():
                        for w in x_copies(p + 1):
                            w.wait()

                    squares((3 - left) * third, third, jnp.where(left == 3, 0.0, scl[...]))

                    @pl.when(left == 1)
                    def _():
                        scales()

            @at(L4 + 2 * TICKS, outer)
            def _(v, n):
                f_copy(v, n).wait_send()

            @at(L5)
            def _(v, n):
                f_copy(v, n).wait_recv()

    lax.fori_loop(0, units + -(-(L4 + 2 * TICKS) // TICKS), step, None)


def _trig(rows):
    half = HEAD // 2
    angle = np.arange(rows, dtype=np.float32)[:, None] * (float(THETA) ** (-np.arange(half) / half)).astype(np.float32)
    angle = angle.astype(np.float64)
    return np.concatenate([np.cos(angle), np.sin(angle)], 1).astype(np.float32)


def _copy(src, dst, buf, s_in, s_out):
    slots, rows = buf.shape[0], buf.shape[1]
    blocks = src.shape[0] // rows

    def at(n):
        return pl.ds(pl.multiple_of(n * rows, rows), rows)

    def read(n):
        return pltpu.make_async_copy(src.at[at(n)], buf.at[lax.rem(n, slots)], s_in.at[lax.rem(n, slots)])

    def write(n):
        return pltpu.make_async_copy(buf.at[lax.rem(n, slots)], dst.at[at(n)], s_out.at[lax.rem(n, slots)])

    ahead = slots // 2
    for n in range(ahead):
        read(n).start()

    def step(n, _):
        @pl.when(n + ahead < blocks)
        def _():
            @pl.when(n + ahead >= slots)
            def _():
                write(n + ahead - slots).wait()

            read(n + ahead).start()

        read(n).wait()
        write(n).start()

    lax.fori_loop(0, blocks, step, None)
    lax.fori_loop(blocks - slots, blocks, lambda n, _: write(n).wait(), None)


def copied(y, rows=32, slots=16):
    dma = pltpu.SemaphoreType.DMA
    rows = min(rows, y.shape[0] // slots)
    return pl.pallas_call(
        _copy,
        out_shape=jax.ShapeDtypeStruct(y.shape, y.dtype),
        in_specs=[pl.BlockSpec(memory_space=pl.ANY)],
        out_specs=pl.BlockSpec(memory_space=pl.ANY),
        scratch_shapes=[pltpu.VMEM((slots, rows, y.shape[1]), y.dtype), dma((slots,)), dma((slots,))],
        compiler_params=pltpu.CompilerParams(vmem_limit_bytes=VMEM),
        name="copied",
    )(y)


def layer(x, gain, wq, wk, wv, wo, chunk=256):
    rows, wide = x.shape
    mine = wq.shape[1]
    heads = mine // HEAD
    kb, nb = wide // PROJ, wide // STEPS
    half = nb // 2
    hbm, vmem = pl.BlockSpec(memory_space=pl.ANY), pl.BlockSpec(memory_space=pltpu.VMEM)

    def slots(n, t=BF16):
        return pltpu.VMEM((n, chunk, half), t)

    def dma(*n):
        return pltpu.SemaphoreType.DMA(n)

    y = pl.pallas_call(
        _kernel,
        out_shape=jax.ShapeDtypeStruct((rows, wide), BF16),
        in_specs=[hbm, vmem, vmem, hbm, hbm, hbm, hbm],
        out_specs=hbm,
        scratch_shapes=[
            pltpu.VMEM((chunk, wide), BF16), pltpu.VMEM((chunk, kb), BF16), pltpu.VMEM((chunk, mine + 2 * HEAD), F32), pltpu.VMEM((chunk, 128), F32),
            pltpu.VMEM((wide // 128, 128), F32),
            pltpu.VMEM((3, kb, mine), BF16), pltpu.VMEM((3, kb, 2 * HEAD), BF16), pltpu.VMEM((3, mine, nb), BF16),
            pltpu.VMEM((heads, chunk, HEAD), BF16), pltpu.VMEM((rows, HEAD), BF16), pltpu.VMEM((HEAD + 16, rows), BF16),
            pltpu.VMEM((2, chunk, mine), BF16), pltpu.VMEM((GROUP // 2, HEAD + 16, 2 * chunk), F32), pltpu.VMEM((8, 2 * chunk), F32),
            slots(2), slots(4), slots(4, F32), slots(2), slots(4), slots(2), slots(4), slots(3), slots(2),
            dma(4), dma(3, 3), dma(3), dma(3), dma(2), dma(4), dma(2, TICKS), dma(4, TICKS), dma(2, TICKS), dma(4, TICKS),
            dma(2, TICKS), dma(2, TICKS), dma(2, TICKS), dma(8, TICKS), dma(2, TICKS), dma(8, TICKS),
        ],
        compiler_params=pltpu.CompilerParams(collective_id=0, has_side_effects=True, vmem_limit_bytes=VMEM),
        cost_estimate=pl.CostEstimate(flops=4 * rows * wide * (mine + HEAD), transcendentals=heads * rows * rows // 2,
                                      bytes_accessed=8 * 4 * wide * mine),
        name="layer",
    )(x, gain.reshape(wide // 128, 128), jnp.asarray(_trig(rows)), wq, wk, wv, wo)
    return copied(y)


def solution(mesh):
    tokens, columns = P("dp", None), P(None, "tp")
    return jax.shard_map(
        layer,
        mesh=mesh,
        in_specs=(tokens, P(None), columns, columns, columns, P("tp", None)),
        out_specs=tokens,
        check_vma=False,
    )
```

```python
import functools

import numpy as np

import jax
import jax.numpy as jnp
from jax import lax
from jax.experimental import pallas as pl
from jax.experimental.pallas import tpu as pltpu
from jax.sharding import PartitionSpec as P

HEAD = 128
THETA = 10000
NEG = -1e30
HIDDEN = 2 * NEG
LOG2E = 1.4426950408889634
MESH = pl.DeviceIdType.MESH
VMEM = 67043328
F32, BF16 = jnp.float32, jnp.bfloat16

STEPS = 12
TICKS = 4
PROJ = 6
GROUP = 4
KEPT = 4
PARTS = 3
QUIET = 2
L1, L2, L3, L4, L5 = 2, 5, 9, 15, 19


def _dot(a, b, ca=1, cb=0):
    return lax.dot_general(a, b, (((ca,), (cb,)), ((), ())), preferred_element_type=F32)


def _kernel(x, gain, trig, wq, wk, wv, wo, y_hbm, y_vmem, wqb, wob, a_s, acc, scl, g_s, wkvb, t_s, q_s, k_s, vt_s, seen, mix, top_s,
            tsend, trecv, own, psend, precv, ssend, mrecv, xres, ybuf,
            sx, sw, swo, sxr, s_t, r_t, s_p, r_p, s_m, r_m, s_yl, s_yp, s_yo, r_y, s_f, r_f, s_trig, s_rq, s_ro):
    rows, wide = x.shape
    chunk = a_s.shape[0]
    heads = wq.shape[1] // HEAD
    chunks = rows // chunk
    early = (chunks - KEPT) * STEPS
    xc = y_vmem.at[pl.ds((KEPT - 1) * chunk, chunk)]
    n_w = wq.shape[1] // PARTS
    kb, nb = wide // PROJ, wide // STEPS
    half = nb // 2
    groups = heads // GROUP
    piece = chunk // TICKS
    units = chunks * STEPS
    e = HEAD**-0.5 * LOG2E

    me = lax.axis_index("tp")
    z, c = lax.div(me, 2), lax.rem(me, 2)
    inner = (z == 1) | (z == 2)
    outer = jnp.logical_not(inner)
    partner = {"tp": 2 * z + 1 - c}
    near = {"tp": 2 * (z + 1 - 2 * lax.rem(z, 2)) + c}
    far = {"tp": 2 * jnp.clip(3 - z, 1, 2) + c}
    rem = lax.rem

    def remote(src, dst, ssem, rsem, to):
        return pltpu.make_async_remote_copy(src_ref=src, dst_ref=dst, send_sem=ssem, recv_sem=rsem, device_id=to, device_id_type=MESH)

    def place(v, n=None):
        r = pl.multiple_of(lax.div(v, STEPS) * chunk, chunk)
        k = pl.multiple_of(rem(v, STEPS) * nb + c * half, half)
        return (pl.ds(r, chunk) if n is None else pl.ds(r + n * piece, piece)), pl.ds(k, half)

    def kept(v, n):
        r = pl.multiple_of(lax.div(v - early, STEPS) * chunk, chunk)
        return y_vmem.at[pl.ds(r + n * piece, piece), place(v)[1]]

    def mine(v, n, late):
        return kept(v, n) if late else y_hbm.at[place(v, n)]

    def either(v, f):
        pl.when(v < early)(lambda: f(False))
        pl.when(v >= early)(lambda: f(True))

    def part_of(n):
        return pl.ds(n * piece, piece)

    def x_copies(p):
        w = wide // 4
        return [pltpu.make_async_copy(x.at[pl.ds(pl.multiple_of(p * chunk, chunk), chunk), pl.ds(n * w, w)], xc.at[:, pl.ds(n * w, w)], sx.at[n])
                for n in range(4)]

    def w_copies(s, n):
        k, b = pl.ds(pl.multiple_of(rem(s, PROJ) * kb, kb), kb), rem(s, 2)
        if n < PARTS:
            at = pl.ds(n * n_w, n_w)
            return [pltpu.make_async_copy(wq.at[k, at], wqb.at[b, :, at], sw.at[n, b])]
        return [pltpu.make_async_copy(wk.at[k, :], wkvb.at[b, :, pl.ds(0, HEAD)], sw.at[n, b]),
                pltpu.make_async_copy(wv.at[k, :], wkvb.at[b, :, pl.ds(HEAD, HEAD)], sw.at[n + 1, b])]

    def start(copies):
        for one in copies:
            one.start()

    def wait(copies):
        for one in copies:
            one.wait()

    def wo_copy(v):
        return pltpu.make_async_copy(wo.at[:, pl.ds(pl.multiple_of(rem(v, STEPS) * nb, nb), nb)], wob.at[rem(v, 2)], swo.at[rem(v, 2)])

    def xres_copy(v):
        r, k = place(v)
        return pltpu.make_async_copy(x.at[r, k], xres.at[rem(v, 3)], sxr.at[rem(v, 3)])

    def t_copy(v):
        return remote(tsend.at[rem(v, 2)], trecv.at[rem(v, 3)], s_t.at[rem(v, 2)], r_t.at[rem(v, 3)], partner)

    def p_copy(v, n):
        k, j = rem(v, 2), rem(v, 4)
        return remote(psend.at[k, part_of(n)], precv.at[j, part_of(n)], s_p.at[k, n], r_p.at[j, n], near)

    def m_copy(v, n):
        k, j = rem(v, 2), rem(v, 3)
        return remote(ssend.at[k, part_of(n)], mrecv.at[j, part_of(n)], s_m.at[k, n], r_m.at[j, n], far)

    def yl_copy(v, n):
        return pltpu.make_async_copy(ybuf.at[rem(v, 2), part_of(n)], mine(v, n, False), s_yl.at[rem(v, 2), n])

    def made(v, n, late):
        return kept(v, n) if late else ybuf.at[rem(v, 2), part_of(n)]

    def yp_copy(v, n, late):
        return remote(made(v, n, late), mine(v, n, late), s_yp.at[rem(v, 2), n], r_f.at[rem(v, 8), n], partner)

    def yo_copy(v, n, late):
        return remote(made(v, n, late), mine(v, n, late), s_yo.at[rem(v, 2), n], r_y.at[rem(v, 8), n], near)

    def f_copy(v, n, late):
        return remote(mine(v, n, late), mine(v, n, late), s_f.at[rem(v, 2), n], r_f.at[rem(v, 8), n], partner)

    def trig_copy(p):
        return pltpu.make_async_copy(trig.at[pl.ds(pl.multiple_of(p * chunk, chunk), chunk), :], t_s, s_trig)

    def refill(b, n):
        k = wqb.shape[2]
        return pltpu.make_async_copy(y_hbm.at[pl.ds(b * chunk, chunk), pl.ds(n * k, k)], wqb.at[b, pl.ds(n * chunk, chunk)], s_rq.at[b, n])

    def refill_wo(b, n):
        k, r = wob.shape[2], chunk // 2
        return pltpu.make_async_copy(y_hbm.at[pl.ds(2 * chunk + b * r, r), pl.ds(n * k, k)], wob.at[b, pl.ds(n * r, r)], s_ro.at[b, n])

    def refills():
        return [refill(b, n) for b in range(2) for n in range(wide // wqb.shape[2])]

    def refills_wo():
        return [refill_wo(b, n) for b in range(2) for n in range(STEPS)]

    def squares(first, count, start):
        def some(n, t):
            v = [xc[:, pl.ds(pl.multiple_of(n * 512, 512) + k * 128, 128)].astype(F32) for k in range(4)]
            return t + ((v[0] * v[0] + v[1] * v[1]) + (v[2] * v[2] + v[3] * v[3]))
        scl[...] = lax.fori_loop(first, first + count, some, start)

    def scales():
        t = jnp.sum(scl[...], axis=1, keepdims=True)
        scl[...] = jnp.broadcast_to(lax.rsqrt(t * (1 / wide) + 1e-6), scl.shape)

    def rotated(t, cos, sin):
        t = t.astype(BF16).astype(F32)
        return (t * cos + pltpu.roll(t, HEAD // 2, 1) * sin).astype(BF16)

    def project(p, i, ticks, ahead=None):
        s = p * PROJ + i
        b = rem(s, 2)
        if 1 in ticks:
            for n in range(kb // 128):
                k = pl.ds(pl.multiple_of(i * kb + n * 128, 128), 128)
                a_s[:, n * 128 : (n + 1) * 128] = (xc[:, k].astype(F32) * scl[...] * g_s[pl.ds(i * (kb // 128) + n, 1), :]).astype(BF16)
            for n in range(PARTS + 1):
                wait(w_copies(s, n))
        for n in [m for t in ticks for m in {1: [0], 2: [1, PARTS], 3: list(range(2, PARTS))}.get(t, [])]:
            at = pl.ds(n * n_w, n_w if n < PARTS else 2 * HEAD)
            d = _dot(a_s[...], wqb[b, :, at] if n < PARTS else wkvb[b])
            acc[:, at] = jnp.where(i == 0, d, acc[:, at] + d)
            if ahead is None:
                pl.when(s + 2 < chunks * PROJ)(lambda: start(w_copies(s + 2, n)))
            elif ahead:
                start(w_copies(s + 2, n))

    def angles():
        cs = t_s[...]
        swapped = pltpu.roll(cs, HEAD // 2, 1)
        low = lax.broadcasted_iota(jnp.int32, cs.shape, 1) < HEAD // 2
        return jnp.where(low, cs, swapped), jnp.where(low, -swapped, cs)

    def queries(group):
        cos, sin = angles()
        for n in range(GROUP):
            q_s[n] = rotated(acc[:, pl.ds(pl.multiple_of((group * GROUP + n) * HEAD, HEAD), HEAD)], cos, sin)

    def keys(p):
        here = pl.ds(pl.multiple_of(p * chunk, chunk), chunk)
        trig_copy(p).wait()
        cos, sin = angles()
        k_s[here, :] = rotated(acc[:, pl.ds(heads * HEAD, HEAD)], cos, sin)
        vt_s[:HEAD, here] = acc[:, pl.ds(heads * HEAD + HEAD, HEAD)].T.astype(BF16)

    strips = range(GROUP // 2)

    def score(j, masked):
        here = pl.ds(pl.multiple_of(j * chunk, chunk), chunk)
        scores = [_dot(k_s[here, :], q_s[pl.ds(2 * n, 2)].reshape(2 * chunk, HEAD), 1, 1) for n in strips]
        if masked:
            query = rem(lax.broadcasted_iota(jnp.int32, scores[0].shape, 1), chunk)
            ok = lax.broadcasted_iota(jnp.int32, scores[0].shape, 0) <= query
            scores = [jnp.where(ok, s, HIDDEN) for s in scores]
        return here, scores

    def block(j, masked):
        here, scores = score(j, masked)
        weights, keeps = [], []
        for n, s in enumerate(scores):
            old = top_s[n : n + 1, :]
            top = jnp.maximum(old, s.max(axis=0, keepdims=True))
            top_s[n : n + 1, :] = top
            weights.append(jnp.exp2((s - top) * e).astype(BF16))
            keeps.append(jnp.exp2((old - top) * e))
        for n, (w, keep) in enumerate(zip(weights, keeps)):
            mix[n] = mix[n] * keep + _dot(vt_s[:, here], w)

    def attended(p, group, sums):
        for n, m in enumerate(sums):
            out = (m[:HEAD, :] * (1 / m[HEAD : HEAD + 1, :])).T.astype(BF16)
            for h in range(2):
                seen[rem(p, 2), :, pl.ds(pl.multiple_of((group * GROUP + 2 * n + h) * HEAD, HEAD), HEAD)] = out[h * chunk : (h + 1) * chunk]

    def attend_first(group, _):
        queries(group)
        here, scores = score(0, True)
        weights = [jnp.exp2((s - s.max(axis=0, keepdims=True)) * e).astype(BF16) for s in scores]
        attended(0, group, [_dot(vt_s[:, here], w) for w in weights])

    xs = x_copies(0)
    start(xs)
    trig_copy(0).start()
    barrier = pltpu.get_barrier_semaphore()
    pl.semaphore_signal(barrier, inc=1, device_id=partner, device_id_type=MESH)
    pl.semaphore_signal(barrier, inc=1, device_id=near, device_id_type=MESH)

    @pl.when(inner)
    def _():
        pl.semaphore_signal(barrier, inc=1, device_id=far, device_id_type=MESH)

    g_s[...] = gain[...].astype(F32)
    vt_s[HEAD:, :] = jnp.ones((vt_s.shape[0] - HEAD, rows), BF16)
    scl[...] = jnp.zeros(scl.shape, F32)
    for n in range(4):
        xs[n].wait()
        if n == 0:
            for m in range(2 * PARTS + 2):
                start(w_copies(m // (PARTS + 1), m % (PARTS + 1)))
        squares(n * (wide // 2048), wide // 2048, scl[...])
    scales()

    lax.fori_loop(0, PROJ - 2, lambda i, _: project(0, i, (1, 2, 3), True), None)
    wo_copy(0).start()
    wo_copy(1).start()
    lax.fori_loop(PROJ - 2, PROJ, lambda i, _: project(0, i, (1, 2, 3), False), None)
    for s in range(PROJ, PROJ + 2) if chunks > 1 else []:
        for m in range(PARTS + 1):
            start(w_copies(s, m))
    start(x_copies(1) if chunks > 1 else [])
    keys(0)
    lax.fori_loop(0, groups, attend_first, None)
    if chunks > 1:
        trig_copy(1).start()

    @pl.when(inner)
    def _():
        pl.semaphore_wait(barrier, 3)

    @pl.when(outer)
    def _():
        pl.semaphore_wait(barrier, 2)

    def step(u, _):
        p, i = lax.div(u, STEPS) + 1, rem(u, STEPS)

        k = jnp.where(p == 1, i - QUIET, i)
        projects = (p < chunks) & (k >= 0) & (k < PROJ)
        left = STEPS - i
        group = jnp.where(p == 1, groups - left, groups - lax.div(left + 1, 2))
        attends = (p < chunks) & (group >= 0)
        share = jnp.where(p == 1, 2, 1)
        adds = (p + 1 < chunks) & (left <= 3)

        pl.when(u == units - STEPS + PROJ + 2)(lambda: start(refills()))
        pl.when(u == units)(lambda: start(refills_wo()))

        for tick in range(TICKS):

            def at(lag, also=None):
                def run(f):
                    v, n = u + (tick - lag) // TICKS, (tick - lag) % TICKS
                    ok = (v >= 0) & (v < units)
                    pl.when(ok if also is None else ok & also)(lambda: f(v, n))
                return run

            if tick == 0:

                @at(TICKS, inner)
                def _(v, n):
                    xres_copy(v).start()

                @at(2 * TICKS)
                def _(v, n):
                    t_copy(v).wait_send()

                @at(0)
                def _(v, n):
                    wo_copy(v).wait()
                    part = pl.ds(pl.multiple_of((1 - c) * half, half), half)
                    tsend[rem(v, 2)] = _dot(seen[rem(lax.div(v, STEPS), 2)], wob[rem(v, 2), :, part]).astype(BF16)
                    t_copy(v).start()

            @at(L1 + 2 * TICKS, outer)
            def _(v, n):
                p_copy(v, n).wait_send()

            @at(L1)
            def _(v, n):
                if n == 0:
                    t_copy(v).wait_recv()
                total = own[rem(v, 3), part_of(n)] + trecv[rem(v, 3), part_of(n)].astype(F32)

                @pl.when(outer)
                def _():
                    psend[rem(v, 2), part_of(n)] = total.astype(BF16)
                    p_copy(v, n).start()

                @pl.when(inner)
                def _():
                    own[rem(v, 3), part_of(n)] = total

            @at(L2 + 2 * TICKS, inner)
            def _(v, n):
                m_copy(v, n).wait_send()

            @at(L2, inner)
            def _(v, n):
                p_copy(v, n).wait_recv()
                ssend[rem(v, 2), part_of(n)] = (own[rem(v, 3), part_of(n)] + precv[rem(v, 4), part_of(n)].astype(F32)).astype(BF16)
                m_copy(v, n).start()

            @at(L3 + 2 * TICKS, inner)
            def _(v, n):
                @functools.partial(either, v)
                def _(late):
                    if not late:
                        yl_copy(v, n).wait()
                    yp_copy(v, n, late).wait_send()
                    yo_copy(v, n, late).wait_send()

            @at(L3, inner)
            def _(v, n):
                if n == 0:
                    xres_copy(v).wait()
                m_copy(v, n).wait_recv()
                total = ssend[rem(v, 2), part_of(n)].astype(F32) + mrecv[rem(v, 3), part_of(n)].astype(F32)
                done = (xres[rem(v, 3), part_of(n)].astype(F32) + total).astype(BF16)

                @functools.partial(either, v)
                def _(late):
                    made(v, n, late)[...] = done
                    yo_copy(v, n, late).start()
                    yp_copy(v, n, late).start()
                    if not late:
                        yl_copy(v, n).start()

            @at(L4, outer)
            def _(v, n):
                @functools.partial(either, v)
                def _(late):
                    yo_copy(v, n, late).wait_recv()
                    f_copy(v, n, late).start()

            if tick == 0:

                @at(0)
                def _(v, n):
                    part = pl.ds(pl.multiple_of(c * half, half), half)
                    own[rem(v, 3)] = _dot(seen[rem(lax.div(v, STEPS), 2)], wob[rem(v, 2), :, part])
                    pl.when(v + 2 < units)(lambda: wo_copy(v + 2).start())

            else:

                @pl.when(projects)
                def _():
                    project(p, k, (tick,))
                    if tick == TICKS - 1:

                        @pl.when(k == PROJ - 1)
                        def _():
                            pl.when(p + 1 < chunks)(lambda: start(x_copies(p + 1)))
                            keys(p)

            @pl.when(attends)
            def _():
                t = jnp.where(p == 1, tick, TICKS * rem(i, 2) + tick) * share
                last = t + share == 2 * TICKS

                if tick == 0:

                    @pl.when(t == 0)
                    def _():
                        queries(group)
                        top_s[...] = jnp.full(top_s.shape, NEG, F32)
                        mix[...] = jnp.zeros(mix.shape, F32)

                lo, hi = lax.div((p + 1) * t, 2 * TICKS), lax.div((p + 1) * (t + share), 2 * TICKS)
                lax.fori_loop(lo, jnp.where(last, p, hi), lambda j, _: block(j, False), None)

                if tick == TICKS - 1:

                    @pl.when(last)
                    def _():
                        block(p, True)
                        attended(p, group, [mix[n] for n in strips])

            if tick == TICKS - 1:
                pl.when((left == 1) & (p + 1 < chunks))(lambda: trig_copy(p + 1).start())

            if tick == TICKS - 1 and chunks > 1:

                @pl.when(u == QUIET - 1)
                def _():
                    wait(x_copies(1))
                    squares(0, wide // 512, jnp.zeros(scl.shape, F32))
                    scales()

            @pl.when(adds)
            def _():
                if tick == 0:

                    @pl.when(left == 3)
                    def _():
                        wait(x_copies(p + 1))
                        scl[...] = jnp.zeros(scl.shape, F32)

                some = wide // 512 // (3 * TICKS)
                squares(((3 - left) * TICKS + tick) * some, some, scl[...])
                if tick == TICKS - 1:
                    pl.when(left == 1)(scales)

            @at(L4 + 2 * TICKS, outer)
            def _(v, n):
                either(v, lambda late: f_copy(v, n, late).wait_send())

            @at(L5)
            def _(v, n):
                either(v, lambda late: f_copy(v, n, late).wait_recv())

    lax.fori_loop(0, units + -(-(L4 + 2 * TICKS) // TICKS), step, None)
    wait(refills() + refills_wo())


def _trig(rows):
    half = HEAD // 2
    angle = np.arange(rows, dtype=np.float32)[:, None] * (float(THETA) ** (-np.arange(half) / half)).astype(np.float32)
    angle = angle.astype(np.float64)
    return np.concatenate([np.cos(angle), np.sin(angle)], 1).astype(np.float32)


def _copy(chunk, src, kept, wqb, wob, dst, buf, s_in, s_out, s_kept, s_q, s_o):
    slots, rows = buf.shape[0], buf.shape[1]
    r = chunk // 2
    first = 2 * chunk + 2 * r
    blocks = (src.shape[0] - first) // rows
    ahead = min(slots // 2, blocks)

    def at(n):
        return pl.ds(pl.multiple_of(first + n * rows, rows), rows)

    def read(n):
        return pltpu.make_async_copy(src.at[at(n)], buf.at[lax.rem(n, slots)], s_in.at[lax.rem(n, slots)])

    def write(n):
        return pltpu.make_async_copy(buf.at[lax.rem(n, slots)], dst.at[at(n)], s_out.at[lax.rem(n, slots)])

    for n in range(ahead):
        read(n).start()
    rest = [pltpu.make_async_copy(kept, dst.at[pl.ds(src.shape[0], kept.shape[0])], s_kept)]
    for b in range(2):
        for n in range(src.shape[1] // wqb.shape[2]):
            k = wqb.shape[2]
            rest.append(pltpu.make_async_copy(wqb.at[b, pl.ds(n * chunk, chunk)], dst.at[pl.ds(b * chunk, chunk), pl.ds(n * k, k)], s_q.at[b, n]))
        for n in range(src.shape[1] // wob.shape[2]):
            k = wob.shape[2]
            rest.append(pltpu.make_async_copy(wob.at[b, pl.ds(n * r, r)], dst.at[pl.ds(2 * chunk + b * r, r), pl.ds(n * k, k)], s_o.at[b, n]))
    for one in rest:
        one.start()

    def step(n, _):
        @pl.when(n + ahead < blocks)
        def _():
            @pl.when(n + ahead >= slots)
            def _():
                write(n + ahead - slots).wait()

            read(n + ahead).start()

        read(n).wait()
        write(n).start()

    lax.fori_loop(0, blocks, step, None)
    lax.fori_loop(max(blocks - slots, 0), blocks, lambda n, _: write(n).wait(), None)
    for one in rest:
        one.wait()


def copied(chunk, y, kept, wqb, wob, rows=32, slots=8):
    dma = pltpu.SemaphoreType.DMA
    wide = y.shape[1]
    rows = min(rows, y.shape[0] // 4 // slots)
    hbm, vmem = pl.BlockSpec(memory_space=pltpu.HBM), pl.BlockSpec(memory_space=pltpu.VMEM)
    kept, wqb, wob = [pltpu.with_memory_space_constraint(t, pltpu.VMEM) for t in (kept, wqb, wob)]
    return pl.pallas_call(
        functools.partial(_copy, chunk),
        out_shape=jax.ShapeDtypeStruct((y.shape[0] + kept.shape[0], wide), y.dtype),
        in_specs=[hbm, vmem, vmem, vmem],
        out_specs=hbm,
        scratch_shapes=[pltpu.VMEM((slots, rows, wide), y.dtype), dma((slots,)), dma((slots,)), dma, dma((2, wide // wqb.shape[2])), dma((2, wide // wob.shape[2]))],
        compiler_params=pltpu.CompilerParams(vmem_limit_bytes=VMEM - 2 * (kept.size + wqb.size + wob.size) - 2**18),
        name="copied",
    )(y, kept, wqb, wob)


def layer(x, gain, wq, wk, wv, wo, chunk=256):
    rows, wide = x.shape
    mine = wq.shape[1]
    heads = mine // HEAD
    kb, nb = wide // PROJ, wide // STEPS
    half = nb // 2
    hbm, vmem = pl.BlockSpec(memory_space=pltpu.HBM), pl.BlockSpec(memory_space=pltpu.VMEM)

    def slots(n, t=BF16):
        return pltpu.VMEM((n, chunk, half), t)

    def dma(*n):
        return pltpu.SemaphoreType.DMA(n)

    late = KEPT * chunk
    y, *kept = pl.pallas_call(
        _kernel,
        out_shape=[jax.ShapeDtypeStruct((rows - late, wide), BF16), pltpu.VMEM((late, wide), BF16),
                   pltpu.VMEM((2, kb, mine), BF16), pltpu.VMEM((2, mine, nb), BF16)],
        in_specs=[hbm, vmem, hbm, hbm, hbm, hbm, hbm],
        out_specs=[hbm, vmem, vmem, vmem],
        scratch_shapes=[
            pltpu.VMEM((chunk, kb), BF16), pltpu.VMEM((chunk, mine + 2 * HEAD), F32), pltpu.VMEM((chunk, 128), F32),
            pltpu.VMEM((wide // 128, 128), F32),
            pltpu.VMEM((2, kb, 2 * HEAD), BF16), pltpu.VMEM((chunk, HEAD), F32),
            pltpu.VMEM((GROUP, chunk, HEAD), BF16), pltpu.VMEM((rows, HEAD), BF16), pltpu.VMEM((HEAD + 16, rows), BF16),
            pltpu.VMEM((2, chunk, mine), BF16), pltpu.VMEM((GROUP // 2, HEAD + 16, 2 * chunk), F32), pltpu.VMEM((8, 2 * chunk), F32),
            slots(2), slots(3), slots(3, F32), slots(2), slots(4), slots(2), slots(3), slots(3), slots(2),
            dma(4), dma(PARTS + 2, 2), dma(2), dma(3), dma(2), dma(3), dma(2, TICKS), dma(4, TICKS), dma(2, TICKS), dma(3, TICKS),
            dma(2, TICKS), dma(2, TICKS), dma(2, TICKS), dma(8, TICKS), dma(2, TICKS), dma(8, TICKS), pltpu.SemaphoreType.DMA, dma(2, wide // mine), dma(2, STEPS),
        ],
        compiler_params=pltpu.CompilerParams(collective_id=0, has_side_effects=True, vmem_limit_bytes=VMEM - 2 * (late * wide + 2 * kb * mine + 2 * mine * nb) - 2**18),
        cost_estimate=pl.CostEstimate(flops=4 * rows * wide * (mine + HEAD), transcendentals=heads * rows * rows // 2,
                                      bytes_accessed=8 * 4 * wide * mine),
        name="layer",
    )(x, gain.reshape(wide // 128, 128), jnp.asarray(_trig(rows)), wq, wk, wv, wo)
    return copied(chunk, y, *kept)


def solution(mesh):
    tokens, columns = P("dp", None), P(None, "tp")
    return jax.shard_map(
        layer,
        mesh=mesh,
        in_specs=(tokens, P(None), columns, columns, columns, P("tp", None)),
        out_specs=tokens,
        check_vma=False,
    )
```

```python
import functools

import numpy as np

import jax
import jax.numpy as jnp
from jax import lax
from jax.experimental import pallas as pl
from jax.experimental.pallas import tpu as pltpu
from jax.sharding import PartitionSpec as P

HEAD = 128
THETA = 10000
NEG = -1e30
HIDDEN = 2 * NEG
LOG2E = 1.4426950408889634
MESH = pl.DeviceIdType.MESH
VMEM = 67043328
F32, BF16 = jnp.float32, jnp.bfloat16

STEPS = 12
TICKS = 4
PROJ = 6
GROUP = 4
KEPT = 4
PARTS = 3
QUIET = 2
L1, L2, L3, L4, L5 = 2, 5, 9, 15, 19


def _dot(a, b, ca=1, cb=0):
    return lax.dot_general(a, b, (((ca,), (cb,)), ((), ())), preferred_element_type=F32)


def _kernel(x, gain, trig, wq, wk, wv, wo, y_hbm, y_vmem, wqb, wob, a_s, acc, scl, g_s, wkvb, t_s, q_s, k_s, vt_s, seen, mix, top_s,
            tsend, trecv, own, psend, precv, ssend, mrecv, xres, ybuf,
            sx, sw, swo, sxr, s_t, r_t, s_p, r_p, s_m, r_m, s_yl, s_yp, s_yo, r_y, s_f, r_f, s_trig, s_rq, s_ro):
    rows, wide = x.shape
    chunk = a_s.shape[0]
    heads = wq.shape[1] // HEAD
    chunks = rows // chunk
    early = (chunks - KEPT) * STEPS
    xc = y_vmem.at[pl.ds((KEPT - 1) * chunk, chunk)]
    n_w = wq.shape[1] // PARTS
    kb, nb = wide // PROJ, wide // STEPS
    half = nb // 2
    groups = heads // GROUP
    piece = chunk // TICKS
    units = chunks * STEPS
    e = HEAD**-0.5 * LOG2E

    me = lax.axis_index("tp")
    z, c = lax.div(me, 2), lax.rem(me, 2)
    inner = (z == 1) | (z == 2)
    outer = jnp.logical_not(inner)
    partner = {"tp": 2 * z + 1 - c}
    near = {"tp": 2 * (z + 1 - 2 * lax.rem(z, 2)) + c}
    far = {"tp": 2 * jnp.clip(3 - z, 1, 2) + c}
    rem = lax.rem

    def remote(src, dst, ssem, rsem, to):
        return pltpu.make_async_remote_copy(src_ref=src, dst_ref=dst, send_sem=ssem, recv_sem=rsem, device_id=to, device_id_type=MESH)

    def place(v, n=None):
        r = pl.multiple_of(lax.div(v, STEPS) * chunk, chunk)
        k = pl.multiple_of(rem(v, STEPS) * nb + c * half, half)
        return (pl.ds(r, chunk) if n is None else pl.ds(r + n * piece, piece)), pl.ds(k, half)

    def kept(v, n):
        r = pl.multiple_of(lax.div(v - early, STEPS) * chunk, chunk)
        return y_vmem.at[pl.ds(r + n * piece, piece), place(v)[1]]

    def mine(v, n, late):
        return kept(v, n) if late else y_hbm.at[place(v, n)]

    def either(v, f):
        pl.when(v < early)(lambda: f(False))
        pl.when(v >= early)(lambda: f(True))

    def part_of(n):
        return pl.ds(n * piece, piece)

    def x_copies(p):
        w = wide // 4
        return [pltpu.make_async_copy(x.at[pl.ds(pl.multiple_of(p * chunk, chunk), chunk), pl.ds(n * w, w)], xc.at[:, pl.ds(n * w, w)], sx.at[n])
                for n in range(4)]

    def w_copies(s, n):
        k, b = pl.ds(pl.multiple_of(rem(s, PROJ) * kb, kb), kb), rem(s, 2)
        if n < PARTS:
            at = pl.ds(n * n_w, n_w)
            return [pltpu.make_async_copy(wq.at[k, at], wqb.at[b, :, at], sw.at[n, b])]
        return [pltpu.make_async_copy(wk.at[k, :], wkvb.at[b, :, pl.ds(0, HEAD)], sw.at[n, b]),
                pltpu.make_async_copy(wv.at[k, :], wkvb.at[b, :, pl.ds(HEAD, HEAD)], sw.at[n + 1, b])]

    def start(copies):
        for one in copies:
            one.start()

    def wait(copies):
        for one in copies:
            one.wait()

    def wo_copy(v):
        return pltpu.make_async_copy(wo.at[:, pl.ds(pl.multiple_of(rem(v, STEPS) * nb, nb), nb)], wob.at[rem(v, 2)], swo.at[rem(v, 2)])

    def xres_copy(v):
        r, k = place(v)
        return pltpu.make_async_copy(x.at[r, k], xres.at[rem(v, 3)], sxr.at[rem(v, 3)])

    def t_copy(v):
        return remote(tsend.at[rem(v, 2)], trecv.at[rem(v, 3)], s_t.at[rem(v, 2)], r_t.at[rem(v, 3)], partner)

    def p_copy(v, n):
        k, j = rem(v, 2), rem(v, 4)
        return remote(psend.at[k, part_of(n)], precv.at[j, part_of(n)], s_p.at[k, n], r_p.at[j, n], near)

    def m_copy(v, n):
        k, j = rem(v, 2), rem(v, 3)
        return remote(ssend.at[k, part_of(n)], mrecv.at[j, part_of(n)], s_m.at[k, n], r_m.at[j, n], far)

    def yl_copy(v, n):
        return pltpu.make_async_copy(ybuf.at[rem(v, 2), part_of(n)], mine(v, n, False), s_yl.at[rem(v, 2), n])

    def made(v, n, late):
        return kept(v, n) if late else ybuf.at[rem(v, 2), part_of(n)]

    def yp_copy(v, n, late):
        return remote(made(v, n, late), mine(v, n, late), s_yp.at[rem(v, 2), n], r_f.at[rem(v, 8), n], partner)

    def yo_copy(v, n, late):
        return remote(made(v, n, late), mine(v, n, late), s_yo.at[rem(v, 2), n], r_y.at[rem(v, 8), n], near)

    def f_copy(v, n, late):
        return remote(mine(v, n, late), mine(v, n, late), s_f.at[rem(v, 2), n], r_f.at[rem(v, 8), n], partner)

    def trig_copy(p):
        return pltpu.make_async_copy(trig.at[pl.ds(pl.multiple_of(p * chunk, chunk), chunk), :], t_s, s_trig)

    def refill(b, n):
        k = wqb.shape[2]
        return pltpu.make_async_copy(y_hbm.at[pl.ds(b * chunk, chunk), pl.ds(n * k, k)], wqb.at[b, pl.ds(n * chunk, chunk)], s_rq.at[b, n])

    def refill_wo(b, n):
        k, r = wob.shape[2], chunk // 2
        return pltpu.make_async_copy(y_hbm.at[pl.ds(2 * chunk + b * r, r), pl.ds(n * k, k)], wob.at[b, pl.ds(n * r, r)], s_ro.at[b, n])

    def refills():
        return [refill(b, n) for b in range(2) for n in range(wide // wqb.shape[2])]

    def refills_wo():
        return [refill_wo(b, n) for b in range(2) for n in range(STEPS)]

    def squares(first, count, start):
        def some(n, t):
            v = [xc[:, pl.ds(pl.multiple_of(n * 512, 512) + k * 128, 128)].astype(F32) for k in range(4)]
            return t + ((v[0] * v[0] + v[1] * v[1]) + (v[2] * v[2] + v[3] * v[3]))
        scl[...] = lax.fori_loop(first, first + count, some, start)

    def scales():
        t = jnp.sum(scl[...], axis=1, keepdims=True)
        scl[...] = jnp.broadcast_to(lax.rsqrt(t * (1 / wide) + 1e-6), scl.shape)

    def rotated(t, cos, sin):
        t = t.astype(BF16).astype(F32)
        return (t * cos + pltpu.roll(t, HEAD // 2, 1) * sin).astype(BF16)

    def project(p, i, ticks, ahead=None):
        s = p * PROJ + i
        b = rem(s, 2)
        if 1 in ticks:
            for n in range(kb // 128):
                k = pl.ds(pl.multiple_of(i * kb + n * 128, 128), 128)
                a_s[:, n * 128 : (n + 1) * 128] = (xc[:, k].astype(F32) * scl[...] * g_s[pl.ds(i * (kb // 128) + n, 1), :]).astype(BF16)
            for n in range(PARTS + 1):
                wait(w_copies(s, n))
        for n in [m for t in ticks for m in {1: [0], 2: [1, PARTS], 3: list(range(2, PARTS))}.get(t, [])]:
            at = pl.ds(n * n_w, n_w if n < PARTS else 2 * HEAD)
            d = _dot(a_s[...], wqb[b, :, at] if n < PARTS else wkvb[b])
            acc[:, at] = jnp.where(i == 0, d, acc[:, at] + d)
            if ahead is None:
                pl.when(s + 2 < chunks * PROJ)(lambda: start(w_copies(s + 2, n)))
            elif ahead:
                start(w_copies(s + 2, n))

    def angles():
        cs = t_s[...]
        swapped = pltpu.roll(cs, HEAD // 2, 1)
        low = lax.broadcasted_iota(jnp.int32, cs.shape, 1) < HEAD // 2
        return jnp.where(low, cs, swapped), jnp.where(low, -swapped, cs)

    def queries(group):
        cos, sin = angles()
        for n in range(GROUP):
            q_s[n] = rotated(acc[:, pl.ds(pl.multiple_of((group * GROUP + n) * HEAD, HEAD), HEAD)], cos, sin)

    def keys(p):
        here = pl.ds(pl.multiple_of(p * chunk, chunk), chunk)
        trig_copy(p).wait()
        cos, sin = angles()
        k_s[here, :] = rotated(acc[:, pl.ds(heads * HEAD, HEAD)], cos, sin)
        vt_s[:HEAD, here] = acc[:, pl.ds(heads * HEAD + HEAD, HEAD)].T.astype(BF16)

    strips = range(GROUP // 2)

    def score(j, masked):
        here = pl.ds(pl.multiple_of(j * chunk, chunk), chunk)
        scores = [_dot(k_s[here, :], q_s[pl.ds(2 * n, 2)].reshape(2 * chunk, HEAD), 1, 1) for n in strips]
        if masked:
            query = rem(lax.broadcasted_iota(jnp.int32, scores[0].shape, 1), chunk)
            ok = lax.broadcasted_iota(jnp.int32, scores[0].shape, 0) <= query
            scores = [jnp.where(ok, s, HIDDEN) for s in scores]
        return here, scores

    def block(j, masked):
        here, scores = score(j, masked)
        weights, keeps = [], []
        for n, s in enumerate(scores):
            old = top_s[n : n + 1, :]
            top = jnp.maximum(old, s.max(axis=0, keepdims=True))
            top_s[n : n + 1, :] = top
            weights.append(jnp.exp2((s - top) * e).astype(BF16))
            keeps.append(jnp.exp2((old - top) * e))
        for n, (w, keep) in enumerate(zip(weights, keeps)):
            mix[n] = mix[n] * keep + _dot(vt_s[:, here], w)

    def attended(p, group, sums):
        for n, m in enumerate(sums):
            out = (m[:HEAD, :] * (1 / m[HEAD : HEAD + 1, :])).T.astype(BF16)
            for h in range(2):
                seen[rem(p, 2), :, pl.ds(pl.multiple_of((group * GROUP + 2 * n + h) * HEAD, HEAD), HEAD)] = out[h * chunk : (h + 1) * chunk]

    def attend_first(group):
        queries(group)
        here, scores = score(0, True)
        weights = [jnp.exp2((s - s.max(axis=0, keepdims=True)) * e).astype(BF16) for s in scores]
        attended(0, group, [_dot(vt_s[:, here], w) for w in weights])

    xs = x_copies(0)
    start(xs)
    trig_copy(0).start()
    barrier = pltpu.get_barrier_semaphore()
    pl.semaphore_signal(barrier, inc=1, device_id=partner, device_id_type=MESH)
    pl.semaphore_signal(barrier, inc=1, device_id=near, device_id_type=MESH)

    @pl.when(inner)
    def _():
        pl.semaphore_signal(barrier, inc=1, device_id=far, device_id_type=MESH)

    g_s[...] = gain[...].astype(F32)
    vt_s[HEAD:, :] = jnp.ones((vt_s.shape[0] - HEAD, rows), BF16)
    scl[...] = jnp.zeros(scl.shape, F32)
    for n in range(4):
        xs[n].wait()
        if n == 0:
            for m in range(2 * PARTS + 2):
                start(w_copies(m // (PARTS + 1), m % (PARTS + 1)))
        squares(n * (wide // 2048), wide // 2048, scl[...])
    scales()

    lax.fori_loop(0, PROJ - 2, lambda i, _: project(0, i, (1, 2, 3), True), None)
    wo_copy(0).start()
    wo_copy(1).start()
    lax.fori_loop(PROJ - 2, PROJ, lambda i, _: project(0, i, (1, 2, 3), False), None)
    for s in range(PROJ, PROJ + 2) if chunks > 1 else []:
        for m in range(PARTS + 1):
            start(w_copies(s, m))
    start(x_copies(1) if chunks > 1 else [])
    keys(0)
    for group in range(groups):
        attend_first(group)
    if chunks > 1:
        trig_copy(1).start()

    @pl.when(inner)
    def _():
        pl.semaphore_wait(barrier, 3)

    @pl.when(outer)
    def _():
        pl.semaphore_wait(barrier, 2)

    def step(u, _):
        p, i = lax.div(u, STEPS) + 1, rem(u, STEPS)

        k = jnp.where(p == 1, i - QUIET, i)
        projects = (p < chunks) & (k >= 0) & (k < PROJ)
        left = STEPS - i
        group = jnp.where(p == 1, groups - left, groups - lax.div(left + 1, 2))
        attends = (p < chunks) & (group >= 0)
        share = jnp.where(p == 1, 2, 1)
        adds = (p + 1 < chunks) & (left <= 3)

        pl.when(u == units - STEPS + PROJ + 2)(lambda: start(refills()))
        pl.when(u == units)(lambda: start(refills_wo()))

        for tick in range(TICKS):

            def at(lag, also=None):
                def run(f):
                    v, n = u + (tick - lag) // TICKS, (tick - lag) % TICKS
                    ok = (v >= 0) & (v < units)
                    pl.when(ok if also is None else ok & also)(lambda: f(v, n))
                return run

            if tick == 0:

                @at(TICKS, inner)
                def _(v, n):
                    xres_copy(v).start()

                @at(2 * TICKS)
                def _(v, n):
                    t_copy(v).wait_send()

                @at(0)
                def _(v, n):
                    wo_copy(v).wait()
                    part = pl.ds(pl.multiple_of((1 - c) * half, half), half)
                    tsend[rem(v, 2)] = _dot(seen[rem(lax.div(v, STEPS), 2)], wob[rem(v, 2), :, part]).astype(BF16)
                    t_copy(v).start()

            @at(L1 + 2 * TICKS, outer)
            def _(v, n):
                p_copy(v, n).wait_send()

            @at(L1)
            def _(v, n):
                if n == 0:
                    t_copy(v).wait_recv()
                total = own[rem(v, 3), part_of(n)] + trecv[rem(v, 3), part_of(n)].astype(F32)

                @pl.when(outer)
                def _():
                    psend[rem(v, 2), part_of(n)] = total.astype(BF16)
                    p_copy(v, n).start()

                @pl.when(inner)
                def _():
                    own[rem(v, 3), part_of(n)] = total

            @at(L2 + 2 * TICKS, inner)
            def _(v, n):
                m_copy(v, n).wait_send()

            @at(L2, inner)
            def _(v, n):
                p_copy(v, n).wait_recv()
                ssend[rem(v, 2), part_of(n)] = (own[rem(v, 3), part_of(n)] + precv[rem(v, 4), part_of(n)].astype(F32)).astype(BF16)
                m_copy(v, n).start()

            @at(L3 + 2 * TICKS, inner)
            def _(v, n):
                @functools.partial(either, v)
                def _(late):
                    if not late:
                        yl_copy(v, n).wait()
                    yp_copy(v, n, late).wait_send()
                    yo_copy(v, n, late).wait_send()

            @at(L3, inner)
            def _(v, n):
                if n == 0:
                    xres_copy(v).wait()
                m_copy(v, n).wait_recv()
                total = ssend[rem(v, 2), part_of(n)].astype(F32) + mrecv[rem(v, 3), part_of(n)].astype(F32)
                done = (xres[rem(v, 3), part_of(n)].astype(F32) + total).astype(BF16)

                @functools.partial(either, v)
                def _(late):
                    made(v, n, late)[...] = done
                    yo_copy(v, n, late).start()
                    yp_copy(v, n, late).start()
                    if not late:
                        yl_copy(v, n).start()

            @at(L4, outer)
            def _(v, n):
                @functools.partial(either, v)
                def _(late):
                    yo_copy(v, n, late).wait_recv()
                    f_copy(v, n, late).start()

            if tick == 0:

                @at(0)
                def _(v, n):
                    part = pl.ds(pl.multiple_of(c * half, half), half)
                    own[rem(v, 3)] = _dot(seen[rem(lax.div(v, STEPS), 2)], wob[rem(v, 2), :, part])
                    pl.when(v + 2 < units)(lambda: wo_copy(v + 2).start())

            else:

                @pl.when(projects)
                def _():
                    project(p, k, (tick,))
                    if tick == TICKS - 1:

                        @pl.when(k == PROJ - 1)
                        def _():
                            pl.when(p + 1 < chunks)(lambda: start(x_copies(p + 1)))
                            keys(p)

            @pl.when(attends)
            def _():
                t = jnp.where(p == 1, tick, TICKS * rem(i, 2) + tick) * share
                last = t + share == 2 * TICKS

                if tick == 0:

                    @pl.when(t == 0)
                    def _():
                        queries(group)
                        top_s[...] = jnp.full(top_s.shape, NEG, F32)
                        mix[...] = jnp.zeros(mix.shape, F32)

                lo, hi = lax.div((p + 1) * t, 2 * TICKS), lax.div((p + 1) * (t + share), 2 * TICKS)
                lax.fori_loop(lo, jnp.where(last, p, hi), lambda j, _: block(j, False), None)

                if tick == TICKS - 1:

                    @pl.when(last)
                    def _():
                        block(p, True)
                        attended(p, group, [mix[n] for n in strips])

            if tick == TICKS - 1:
                pl.when((left == 1) & (p + 1 < chunks))(lambda: trig_copy(p + 1).start())

            if tick == TICKS - 1 and chunks > 1:

                @pl.when(u == QUIET - 1)
                def _():
                    wait(x_copies(1))
                    squares(0, wide // 512, jnp.zeros(scl.shape, F32))
                    scales()

            @pl.when(adds)
            def _():
                if tick == 0:

                    @pl.when(left == 3)
                    def _():
                        wait(x_copies(p + 1))
                        scl[...] = jnp.zeros(scl.shape, F32)

                some = wide // 512 // (3 * TICKS)
                squares(((3 - left) * TICKS + tick) * some, some, scl[...])
                if tick == TICKS - 1:
                    pl.when(left == 1)(scales)

            @at(L4 + 2 * TICKS, outer)
            def _(v, n):
                either(v, lambda late: f_copy(v, n, late).wait_send())

            @at(L5)
            def _(v, n):
                either(v, lambda late: f_copy(v, n, late).wait_recv())

    lax.fori_loop(0, units + -(-(L4 + 2 * TICKS) // TICKS), step, None)
    wait(refills() + refills_wo())


def _trig(rows):
    half = HEAD // 2
    angle = np.arange(rows, dtype=np.float32)[:, None] * (float(THETA) ** (-np.arange(half) / half)).astype(np.float32)
    angle = angle.astype(np.float64)
    return np.concatenate([np.cos(angle), np.sin(angle)], 1).astype(np.float32)


def _copy(chunk, src, kept, wqb, wob, dst, buf, s_in, s_out, s_kept, s_q, s_o):
    slots, rows = buf.shape[0], buf.shape[1]
    r = chunk // 2
    first = 2 * chunk + 2 * r
    blocks = (src.shape[0] - first) // rows
    ahead = min(slots // 2, blocks)

    def at(n):
        return pl.ds(pl.multiple_of(first + n * rows, rows), rows)

    def read(n):
        return pltpu.make_async_copy(src.at[at(n)], buf.at[lax.rem(n, slots)], s_in.at[lax.rem(n, slots)])

    def write(n):
        return pltpu.make_async_copy(buf.at[lax.rem(n, slots)], dst.at[at(n)], s_out.at[lax.rem(n, slots)])

    for n in range(ahead):
        read(n).start()
    rest = [pltpu.make_async_copy(kept, dst.at[pl.ds(src.shape[0], kept.shape[0])], s_kept)]
    for b in range(2):
        for n in range(src.shape[1] // wqb.shape[2]):
            k = wqb.shape[2]
            rest.append(pltpu.make_async_copy(wqb.at[b, pl.ds(n * chunk, chunk)], dst.at[pl.ds(b * chunk, chunk), pl.ds(n * k, k)], s_q.at[b, n]))
        for n in range(src.shape[1] // wob.shape[2]):
            k = wob.shape[2]
            rest.append(pltpu.make_async_copy(wob.at[b, pl.ds(n * r, r)], dst.at[pl.ds(2 * chunk + b * r, r), pl.ds(n * k, k)], s_o.at[b, n]))
    for one in rest:
        one.start()

    def step(n, _):
        @pl.when(n + ahead < blocks)
        def _():
            @pl.when(n + ahead >= slots)
            def _():
                write(n + ahead - slots).wait()

            read(n + ahead).start()

        read(n).wait()
        write(n).start()

    lax.fori_loop(0, blocks, step, None)
    lax.fori_loop(max(blocks - slots, 0), blocks, lambda n, _: write(n).wait(), None)
    for one in rest:
        one.wait()


def copied(chunk, y, kept, wqb, wob, rows=32, slots=8):
    dma = pltpu.SemaphoreType.DMA
    wide = y.shape[1]
    rows = min(rows, y.shape[0] // 4 // slots)
    hbm, vmem = pl.BlockSpec(memory_space=pltpu.HBM), pl.BlockSpec(memory_space=pltpu.VMEM)
    kept, wqb, wob = [pltpu.with_memory_space_constraint(t, pltpu.VMEM) for t in (kept, wqb, wob)]
    return pl.pallas_call(
        functools.partial(_copy, chunk),
        out_shape=jax.ShapeDtypeStruct((y.shape[0] + kept.shape[0], wide), y.dtype),
        in_specs=[hbm, vmem, vmem, vmem],
        out_specs=hbm,
        scratch_shapes=[pltpu.VMEM((slots, rows, wide), y.dtype), dma((slots,)), dma((slots,)), dma, dma((2, wide // wqb.shape[2])), dma((2, wide // wob.shape[2]))],
        compiler_params=pltpu.CompilerParams(vmem_limit_bytes=VMEM - 2 * (kept.size + wqb.size + wob.size) - 2**18),
        name="copied",
    )(y, kept, wqb, wob)


def layer(x, gain, wq, wk, wv, wo, chunk=256):
    rows, wide = x.shape
    mine = wq.shape[1]
    heads = mine // HEAD
    kb, nb = wide // PROJ, wide // STEPS
    half = nb // 2
    hbm, vmem = pl.BlockSpec(memory_space=pltpu.HBM), pl.BlockSpec(memory_space=pltpu.VMEM)

    def slots(n, t=BF16):
        return pltpu.VMEM((n, chunk, half), t)

    def dma(*n):
        return pltpu.SemaphoreType.DMA(n)

    late = KEPT * chunk
    y, *kept = pl.pallas_call(
        _kernel,
        out_shape=[jax.ShapeDtypeStruct((rows - late, wide), BF16), pltpu.VMEM((late, wide), BF16),
                   pltpu.VMEM((2, kb, mine), BF16), pltpu.VMEM((2, mine, nb), BF16)],
        in_specs=[hbm, vmem, hbm, hbm, hbm, hbm, hbm],
        out_specs=[hbm, vmem, vmem, vmem],
        scratch_shapes=[
            pltpu.VMEM((chunk, kb), BF16), pltpu.VMEM((chunk, mine + 2 * HEAD), F32), pltpu.VMEM((chunk, 128), F32),
            pltpu.VMEM((wide // 128, 128), F32),
            pltpu.VMEM((2, kb, 2 * HEAD), BF16), pltpu.VMEM((chunk, HEAD), F32),
            pltpu.VMEM((GROUP, chunk, HEAD), BF16), pltpu.VMEM((rows, HEAD), BF16), pltpu.VMEM((HEAD + 16, rows), BF16),
            pltpu.VMEM((2, chunk, mine), BF16), pltpu.VMEM((GROUP // 2, HEAD + 16, 2 * chunk), F32), pltpu.VMEM((8, 2 * chunk), F32),
            slots(2), slots(3), slots(3, F32), slots(2), slots(4), slots(2), slots(3), slots(3), slots(2),
            dma(4), dma(PARTS + 2, 2), dma(2), dma(3), dma(2), dma(3), dma(2, TICKS), dma(4, TICKS), dma(2, TICKS), dma(3, TICKS),
            dma(2, TICKS), dma(2, TICKS), dma(2, TICKS), dma(8, TICKS), dma(2, TICKS), dma(8, TICKS), pltpu.SemaphoreType.DMA, dma(2, wide // mine), dma(2, STEPS),
        ],
        compiler_params=pltpu.CompilerParams(collective_id=0, has_side_effects=True, vmem_limit_bytes=VMEM - 2 * (late * wide + 2 * kb * mine + 2 * mine * nb) - 2**18),
        cost_estimate=pl.CostEstimate(flops=4 * rows * wide * (mine + HEAD), transcendentals=heads * rows * rows // 2,
                                      bytes_accessed=8 * 4 * wide * mine),
        name="layer",
    )(x, gain.reshape(wide // 128, 128), jnp.asarray(_trig(rows)), wq, wk, wv, wo)
    return copied(chunk, y, *kept)


def solution(mesh):
    tokens, columns = P("dp", None), P(None, "tp")
    return jax.shard_map(
        layer,
        mesh=mesh,
        in_specs=(tokens, P(None), columns, columns, columns, P("tp", None)),
        out_specs=tokens,
        check_vma=False,
    )
```
